32 devices in a mesh: dp: 4 (over y, x), vocab: 8 (over z, core).
Axes of the slice: x: 2, y: 2, z: 4, core: 2. Of those that a mesh axis runs over, the one named last changes fastest.
Arguments:
- hidden: bfloat16 [1024, 8192], P('dp'), may hold values from -14 to 14
- weight: bfloat16 [8192, 8192], P('dp', 'vocab'), may hold values from -1 to 1, as said below
- targets: int32 [1024], P('dp'), may hold values from 0 to 8191
- cotangent: float32 [1024], P('dp'), may hold values from 1 to 8
Outputs:
- loss: float32 [1024], P('dp')
- grad_hidden: bfloat16 [1024, 8192], P('vocab', 'dp')
- grad_weight: bfloat16 [8192, 8192], P('dp', 'vocab')
The draws below stay inside these ranges and needn't reach their ends.
Inputs may be any that keep to these rules, and one draw needn't show every extreme that they name: `weight`: entries drawn with standard deviation 4 / sqrt(8192).
All inputs are finite; a program needn't handle non-finite values.
Results may differ from the reference program's by a relative error of at most 0.0047.
Values may be sent and summed in bfloat16 or wider, within the bound.
No kernel may reach another device: no remote copies, remote signals or barrier semaphores. Data moves between devices by JAX's collectives and lax.ppermute only.
A program may use at most 128 MiB of HBM per device.

```python
import math
import jax
import jax.numpy as jnp
from jax import lax

D = 8192
VOCAB = 8192
TOKENS = 1024


def joint_draw(key):
    weight_key = jax.random.fold_in(key, 11)
    hidden_key = jax.random.fold_in(key, 12)
    weight = jnp.clip(jnp.clip(jax.random.normal(weight_key, (D, VOCAB), jnp.float32), -6.0, 6.0) * (4.0 / D ** 0.5), -1.0, 1.0)
    hidden = jnp.clip(jax.random.normal(hidden_key, (TOKENS, D), jnp.float32), -6.0, 6.0)
    return (weight, hidden)


def draw_weight(key, part):
    weight, hidden = joint_draw(key)
    return weight.astype(jnp.bfloat16)


def draw_hidden(key, part):
    weight, hidden = joint_draw(key)
    return hidden.astype(jnp.bfloat16)


def set_ends(result, key, smallest, top_value):
    longest = result.shape.index(max(result.shape))
    spots = []
    for shift in (0, 1):
        where = [jax.random.randint(jax.random.fold_in(key, axis), (), 0, length) for axis, length in enumerate(result.shape)]
        where[longest] = (where[longest] + shift) % result.shape[longest]
        spots.append(tuple(where))
    return result.at[spots[0]].set(smallest).at[spots[1]].set(top_value)


def shard_levels(own_key, dims, split, smallest, top_value):
    def one(position, shards_of):
        steps = jax.random.uniform(jax.random.fold_in(jax.random.fold_in(own_key, 6), position), (shards_of,), jnp.float32, smallest / len(split), top_value / len(split))
        return jnp.repeat(jnp.exp(steps), dims[position] // shards_of).reshape((-1,) + (1,) * (len(dims) - position - 1))

    gain = one(*split[0])
    for cut in split[1:]:
        gain = gain * one(*cut)
    return gain


def setup_inputs(seed: int = 0) -> dict:
    key_list = jax.random.split(jax.random.key(seed), 5)
    return {
        "hidden": draw_hidden(jax.random.fold_in(key_list[4], 71), 0),
        "weight": draw_weight(jax.random.fold_in(key_list[4], 71), 0),
        "targets": set_ends(jax.random.randint(key_list[2], (TOKENS,), 0, VOCAB), jax.random.fold_in(key_list[2], 1), 0, VOCAB - 1).astype(jnp.int32),
        "cotangent": jnp.clip(jnp.exp(math.log(8.0) - 2.0794415 * jax.random.uniform(key_list[3], (TOKENS,), jnp.float32) ** shard_levels(key_list[3], (TOKENS,), ((0, 4),), -0.2, 0.2)), 1.0, 8.0),
    }


def reference(hidden, weight, targets, cotangent):
    logits = jnp.dot(hidden, weight, preferred_element_type=jnp.float32)
    row_max = jnp.max(logits, axis=1, keepdims=True)
    shifted = jnp.exp(logits - row_max)
    sum_exp = jnp.sum(shifted, axis=1, keepdims=True)
    columns = jnp.arange(VOCAB, dtype=jnp.int32)
    onehot = (targets.astype(jnp.int32)[:, None] == columns[None, :]).astype(jnp.float32)
    picked = jnp.sum(logits * onehot, axis=1)
    loss = row_max[:, 0] + jnp.log(sum_exp[:, 0]) - picked
    grad_logits = (cotangent[:, None] * (shifted / sum_exp - onehot)).astype(jnp.bfloat16)
    grad_hidden = lax.dot_general(grad_logits, weight, (((1,), (1,)), ((), ())), preferred_element_type=jnp.float32).astype(jnp.bfloat16)
    grad_weight = lax.dot_general(hidden, grad_logits, (((0,), (0,)), ((), ())), preferred_element_type=jnp.float32).astype(jnp.bfloat16)
    return (loss, grad_hidden, grad_weight)
```

```python
import jax
import jax.numpy as jnp
from jax import lax
from jax.sharding import Mesh, PartitionSpec as P

CORES = 2


def forward_dot(rows, weight):
    return jnp.dot(rows, weight, preferred_element_type=jnp.float32)


def hidden_dot(grads, weight):
    return lax.dot_general(grads, weight, (((1,), (1,)), ((), ())), preferred_element_type=jnp.float32)


def shards(hidden, weight, targets, cotangent):
    dp, deep = lax.axis_size("dp"), lax.axis_size("z")
    own, vocab_width = hidden.shape[0], weight.shape[1]
    block = own * dp // (deep * CORES)
    core = lax.axis_index("core")
    swap = [(0, 1), (1, 0)]

    def halves(x):
        parts = x.reshape((own // (CORES * block), CORES, block) + x.shape[1:])
        pick = lambda c: lax.dynamic_index_in_dim(parts, c, 1, keepdims=False).reshape((own // CORES,) + x.shape[1:])
        return pick(core), pick(1 - core)

    mine = lax.all_to_all(halves(hidden)[0], "dp", split_axis=1, concat_axis=0, tiled=True)
    other = lax.ppermute(mine, "core", swap)
    half = mine.shape[0]

    def scatter(part):
        return lax.psum_scatter(part, "dp", scatter_dimension=0, tiled=True)

    both = jnp.concatenate([forward_dot(mine, weight).reshape(dp, 1, half // dp, vocab_width), forward_dot(other, weight).reshape(dp, 1, half // dp, vocab_width)], axis=1)
    logits = scatter(both.reshape(2 * half, vocab_width)).reshape(2, half // dp, vocab_width)
    goal = jnp.stack(halves(targets))
    cot = jnp.stack(halves(cotangent))
    first = (lax.axis_index("z") * CORES + core) * vocab_width
    onehot = (goal[:, :, None] == first + lax.iota(jnp.int32, vocab_width)).astype(jnp.float32)
    local_max = jnp.max(logits, axis=2)
    shifted = jnp.exp(logits - local_max[:, :, None])
    local = jnp.stack([local_max, jnp.sum(shifted, axis=2), jnp.sum(logits * onehot, axis=2)])
    order = jnp.where(core == 0, local, local[:, ::-1])
    every = lax.all_gather(order, ("z", "core"), axis=0)
    maxima = every[:, 0]
    row_max = jnp.max(maxima, axis=0)
    sum_exp = jnp.sum(every[:, 1] * jnp.exp(maxima - row_max), axis=0)
    loss = row_max + jnp.log(sum_exp) - jnp.sum(every[:, 2], axis=0)
    loss = loss.reshape(CORES, own // (CORES * block), block).swapaxes(0, 1).reshape(own)
    turn = lambda x: jnp.where(core == 0, x, x[::-1])
    row_max, sum_exp = turn(row_max), turn(sum_exp)
    scale = jnp.exp(local_max - row_max) / sum_exp
    grads = (cot[:, :, None] * (shifted * scale[:, :, None] - onehot)).astype(jnp.bfloat16)
    gathered = lax.all_gather(grads, "dp", axis=0, tiled=False)
    mine_grads = gathered[:, 0].reshape(half, vocab_width)
    other_grads = gathered[:, 1].reshape(half, vocab_width)
    away = lax.ppermute(hidden_dot(other_grads, weight).astype(jnp.bfloat16), "core", swap)
    part = hidden_dot(mine_grads, weight) + away.astype(jnp.float32)
    grad_hidden = lax.psum_scatter(part.astype(jnp.bfloat16), "z", scatter_dimension=0, tiled=True)
    weigh = lambda h, g: lax.dot_general(h, g, (((0,), (0,)), ((), ())), preferred_element_type=jnp.float32)
    rows = jnp.concatenate([mine, other])
    grad_weight = weigh(rows, jnp.concatenate([mine_grads, other_grads])).astype(jnp.bfloat16)
    return (loss, grad_hidden, grad_weight)


def solution(mesh):
    dp, vocab = mesh.shape["dp"], mesh.shape["vocab"]
    fine = Mesh(mesh.devices.reshape(dp, vocab // CORES, CORES), ("dp", "z", "core"))
    cols = ("z", "core")
    in_specs = (P("dp", None), P("dp", cols), P("dp"), P("dp"))
    out_specs = (P("dp"), P(cols, "dp"), P("dp", cols))
    return jax.shard_map(shards, mesh=fine, in_specs=in_specs, out_specs=out_specs, check_vma=False)
```

```python
import jax
import jax.numpy as jnp
from jax import lax
from jax.sharding import Mesh, PartitionSpec as P

CORES = 2


def forward_dot(rows, weight):
    return jnp.dot(rows, weight, preferred_element_type=jnp.float32)


def hidden_dot(grads, weight):
    return lax.dot_general(grads, weight, (((1,), (1,)), ((), ())), preferred_element_type=jnp.float32)


def shards(hidden, weight, targets, cotangent):
    dp, deep = lax.axis_size("dp"), lax.axis_size("z")
    own, vocab_width = hidden.shape[0], weight.shape[1]
    block = own * dp // (deep * CORES)
    core = lax.axis_index("core")
    swap = [(0, 1), (1, 0)]

    def halves(x):
        parts = x.reshape((own // (CORES * block), CORES, block) + x.shape[1:])
        pick = lambda c: lax.dynamic_index_in_dim(parts, c, 1, keepdims=False).reshape((own // CORES,) + x.shape[1:])
        return pick(core), pick(1 - core)

    me = lax.axis_index("dp")
    width = weight.shape[0]

    def swing(x, k):
        return lax.ppermute(x, "dp", [(i, i ^ k) for i in range(dp)])

    share = halves(hidden)[0]

    def column_block(k):
        return lax.dynamic_slice_in_dim(share, (me ^ k) * width, width, axis=1)

    mine = [column_block(0)] + [swing(column_block(k), k) for k in range(1, dp)]
    other = [lax.ppermute(x, "core", swap) for x in mine]
    part_rows = mine[0].shape[0]

    def partials(blocks, bit):
        sets = [[k for k in range(dp) if bool(k & bit) == flag] for flag in (True, False)]
        made = [None] * dp
        for keys in sets:
            out = forward_dot(jnp.concatenate([blocks[k] for k in keys]), weight)
            for n, k in enumerate(keys):
                made[k] = out[n * part_rows:(n + 1) * part_rows]
        return made

    bits = [1 << n for n in range(dp.bit_length() - 1)]

    def reduce_blocks(blocks, order):
        held = dict(enumerate(partials(blocks, order[0])))
        for bit in order:
            sent = {k: swing(held[k], bit) for k in held if k & bit}
            held = {k: held[k] + sent[k | bit] for k in held if not k & bit}
        return held[0]

    logits = jnp.stack([reduce_blocks(mine, bits), reduce_blocks(other, bits[::-1])])
    goal = jnp.stack(halves(targets))
    cot = jnp.stack(halves(cotangent))
    first = (lax.axis_index("z") * CORES + core) * vocab_width
    onehot = (goal[:, :, None] == first + lax.iota(jnp.int32, vocab_width)).astype(jnp.float32)
    local_max = jnp.max(logits, axis=2)
    shifted = jnp.exp(logits - local_max[:, :, None])
    local = jnp.stack([local_max, jnp.sum(shifted, axis=2), jnp.sum(logits * onehot, axis=2)])
    depth = lax.axis_index("z")
    partner = lax.ppermute(local, "core", swap)[:, ::-1]
    pair = jnp.where(core == 0, jnp.stack([local, partner]), jnp.stack([partner, local]))
    pair_max = jnp.max(pair[:, 0], axis=0)
    pair_sum = jnp.sum(pair[:, 1] * jnp.exp(pair[:, 0] - pair_max), axis=0)
    merged = jnp.stack([pair_max, pair_sum, jnp.sum(pair[:, 2], axis=0)])
    ring = jnp.stack([merged] + [lax.ppermute(merged, "z", [((i + n) % deep, i) for i in range(deep)]) for n in range(1, deep)])
    every = jnp.stack([lax.dynamic_index_in_dim(ring, (i - depth) % deep, 0, keepdims=False) for i in range(deep)])
    maxima = every[:, 0]
    row_max = jnp.max(maxima, axis=0)
    sum_exp = jnp.sum(every[:, 1] * jnp.exp(maxima - row_max), axis=0)
    loss = row_max + jnp.log(sum_exp) - jnp.sum(every[:, 2], axis=0)
    loss = jnp.where(core == 0, loss, loss[::-1])
    loss = loss.reshape(CORES, own // (CORES * block), block).swapaxes(0, 1).reshape(own)
    scale = jnp.exp(local_max - row_max) / sum_exp
    grads = (cot[:, :, None] * (shifted * scale[:, :, None] - onehot)).astype(jnp.bfloat16)

    def spread_out(block, order):
        held = {0: block}
        for bit in order:
            held.update({k | bit: swing(x, bit) for k, x in list(held.items())})
        return [held[k] for k in range(dp)]

    other_grads = spread_out(grads[1], bits[::-1])
    mine_grads = spread_out(grads[0], bits)
    near_mine, near_other = jnp.stack(mine_grads), jnp.stack(other_grads)
    per = deep // dp

    def chunk(near, r):
        d = (depth + r) % deep
        return lax.dynamic_slice(near, (me ^ (d // per), (d % per) * block, 0), (1, block, vocab_width))[0]

    def share_of(r):
        away = lax.ppermute(hidden_dot(chunk(near_other, r), weight), "core", swap)
        return hidden_dot(chunk(near_mine, r), weight) + away

    shares = {}
    for n in range(1, deep // 2 + 1):
        for r in (deep - n, n):
            if r not in shares:
                shares[r] = share_of(r)
    shares[0] = share_of(0)
    cut = width // 2
    ups, downs = [(i, (i + 1) % deep) for i in range(deep)], [(i, (i - 1) % deep) for i in range(deep)]
    up, down = shares[deep - 1][:, :cut], shares[1][:, cut:]
    for n in range(1, deep):
        up = lax.ppermute(up.astype(jnp.bfloat16), "z", ups).astype(jnp.float32) + shares[(deep - 1 - n) % deep][:, :cut]
        down = lax.ppermute(down.astype(jnp.bfloat16), "z", downs).astype(jnp.float32) + shares[(1 + n) % deep][:, cut:]
    grad_hidden = jnp.concatenate([up, down], axis=1).astype(jnp.bfloat16)
    weigh = lambda h, g: lax.dot_general(h, g, (((0,), (0,)), ((), ())), preferred_element_type=jnp.float32)
    rows = jnp.concatenate(mine + other)
    columns = jnp.concatenate(mine_grads + other_grads)
    grad_weight = weigh(rows, columns).astype(jnp.bfloat16)
    return (loss, grad_hidden, grad_weight)


def solution(mesh):
    dp, vocab = mesh.shape["dp"], mesh.shape["vocab"]
    fine = Mesh(mesh.devices.reshape(dp, vocab // CORES, CORES), ("dp", "z", "core"))
    cols = ("z", "core")
    in_specs = (P("dp", None), P("dp", cols), P("dp"), P("dp"))
    out_specs = (P("dp"), P(cols, "dp"), P("dp", cols))
    return jax.shard_map(shards, mesh=fine, in_specs=in_specs, out_specs=out_specs, check_vma=False)
```
